32 devices in a mesh: member: 4 (over y, core), mesh: 8 (over z, x).
Axes of the slice: x: 2, y: 2, z: 4, core: 2. Of those that a mesh axis runs over, the one named last changes fastest.
Arguments:
- hidden_embedding: bfloat16 [8, 4096, 512], P('member', 'mesh'), may hold values from -6 to 6
- decoder_matrix: bfloat16 [512, 96], replicated, may hold values from -0.25 to 0.25
- baseline_field: float32 [96, 4096], P(None, 'mesh'), may hold values from -6 to 6
- truth_field: float32 [96, 4096], P(None, 'mesh'), may hold values from -6 to 6
- cell_surface_share: float32 [4096], P('mesh'), may hold values from 0.3 to 3
- node_order: int32 [8, 512], P('mesh'), may hold values from 0 to 511, each once within a row
- query: bfloat16 [8, 4096, 512], P('member', 'mesh'), may hold values from -6 to 6
- key_rows: bfloat16 [8, 4096, 512], P('member', 'mesh'), may hold values from -6 to 6
- value_rows: bfloat16 [8, 4096, 512], P('member', 'mesh'), may hold values from -6 to 6
- row_lse: float32 [8, 8, 4096], P('member', None, 'mesh'), may hold values from 6.5 to 8.5
- kv_owner: int32 [8, 8], replicated, may hold values from 0 to 7, each once within a row
- kv_local: int32 [8, 8], replicated, may hold values from 0 to 3
Outputs:
- grad_query: float32 [8, 4096, 512], P('member', 'mesh')
- grad_key: float32 [8, 4096, 512], P('member', 'mesh')
- grad_value: float32 [8, 4096, 512], P('member', 'mesh')
The draws below stay inside these ranges and needn't reach their ends.
Inputs may be any that keep to these rules, and one draw needn't show every extreme that they name: `kv_owner`: each row names every shard once. `node_order`: each row holds every number of 0 to 511 once.
All inputs are finite; a program needn't handle non-finite values.
Results may differ from the reference program's by a relative error of at most 0.0068.
Values may be sent and summed in bfloat16 or wider, within the bound.
A program may use at most 128 MiB of HBM per device.

```python
import math
import jax
import jax.numpy as jnp
import numpy as np
from jax import lax

CH = 96
HEADS = 8
NODE_DEV = 512
KB = 128
KNB = 8
WIDTH = 512
KBLK_DEV = 4
SHARDS = 8
NODES = 4096
MEMBERS = 8


def with_ends(array, key, low, top_value):
    place = [jax.random.randint(jax.random.fold_in(key, axis), (), 0, length) for axis, length in enumerate(array.shape)]
    longest = array.shape.index(max(array.shape))
    neighbour = place[:longest] + [(place[longest] + 1) % array.shape[longest]] + place[longest + 1:]
    return array.at[tuple(place)].set(low).at[tuple(neighbour)].set(top_value)


def shard_levels(own_key, dims, split, least, high):
    level, own = 1.0, jax.random.fold_in(own_key, 6)
    for axis_at, parts in split:
        heights = jnp.exp(jax.random.uniform(jax.random.fold_in(own, axis_at), (parts,), jnp.float32, least / len(split), high / len(split)))
        level = level * jnp.repeat(heights, dims[axis_at] // parts).reshape([-1 if axis == axis_at else 1 for axis in range(len(dims))])
    return level


def cumulative_ranks(number_of, slope):
    weights = [(1 << 20) // math.isqrt(grade ** slope) + 1 for grade in range(1, number_of + 1)]
    deviation = 1 + sum(weights) // (1 << 30)
    return np.cumsum(np.array([max(1, weight // deviation) for weight in weights]))


def ranked_ids(rng, extent, count, lean):
    listing = cumulative_ranks(count, lean)
    ticket = jax.random.randint(jax.random.fold_in(rng, 1), extent, 0, int(listing[count - 1]))
    grade = jnp.searchsorted(jnp.asarray(listing, jnp.int32), ticket, side="right")
    return jax.random.permutation(jax.random.fold_in(rng, 2), count)[grade].astype(jnp.int32)


def noise(key, shape, width, bound, shards=(), kind=jnp.bfloat16):
    factor_of = shard_levels(key, shape, shards, -0.22, 0.18) if shards else 1.0
    values = jax.random.normal(key, shape, jnp.float32) * width * factor_of
    return jnp.minimum(jnp.maximum(values, -bound), bound).astype(kind)


def setup_inputs(seed: int = 0) -> dict:
    streams_of = jax.random.split(jax.random.key(seed), 13)
    hidden_embedding = noise(streams_of[0], (MEMBERS, NODES, WIDTH), 1.0, 6.0, ((0, 4), (1, 8)))
    decoder_matrix = noise(streams_of[1], (WIDTH, CH), WIDTH ** -0.5, 0.25)
    baseline_field = noise(streams_of[2], (CH, NODES), 1.0, 6.0, ((1, 8),), jnp.float32)
    truth_field = noise(streams_of[3], (CH, NODES), 1.0, 6.0, ((1, 8),), jnp.float32)
    cell_surface_share = jnp.clip(jnp.exp(math.log(3.0) - 2.3025851 * jax.random.uniform(streams_of[4], (NODES,), jnp.float32) ** shard_levels(streams_of[4], (NODES,), ((0, 8),), -0.2, 0.2)), 0.3, 3.0)
    node_order = jax.vmap(lambda own: jax.random.permutation(own, NODE_DEV))(jax.random.split(streams_of[5], SHARDS)).reshape((SHARDS, NODE_DEV)).astype(jnp.int32)
    query = noise(streams_of[6], (MEMBERS, NODES, WIDTH), 1.0, 6.0, ((0, 4), (1, 8)))
    key_rows = noise(streams_of[7], (MEMBERS, NODES, WIDTH), 1.0, 6.0, ((0, 4), (1, 8)))
    value_rows = noise(streams_of[8], (MEMBERS, NODES, WIDTH), 1.0, 6.0, ((0, 4), (1, 8)))
    row_lse = jnp.clip(6.5 + 2.0 * jax.random.uniform(streams_of[9], (MEMBERS, HEADS, NODES), jnp.float32) ** shard_levels(streams_of[9], (MEMBERS, HEADS, NODES), ((0, 4), (2, 8)), -0.2, 0.2), 6.5, 8.5)
    kv_owner = jax.vmap(lambda own: jax.random.permutation(own, SHARDS))(jax.random.split(streams_of[10], SHARDS)).reshape((SHARDS, KNB)).astype(jnp.int32)
    kv_local = with_ends(ranked_ids(streams_of[11], (SHARDS, KNB), KBLK_DEV, 2), jax.random.fold_in(streams_of[11], 3), 0, KBLK_DEV - 1).astype(jnp.int32)
    return {"hidden_embedding": hidden_embedding, "decoder_matrix": decoder_matrix, "baseline_field": baseline_field, "truth_field": truth_field, "cell_surface_share": cell_surface_share, "node_order": node_order, "query": query, "key_rows": key_rows, "value_rows": value_rows, "row_lse": row_lse, "kv_owner": kv_owner, "kv_local": kv_local}


LOSS_SCALE = 4096.0
FAIR_EPS = 0.05
NORM_EPS = 1e-06

def unit_scaled_lines(differences):
    return differences / jnp.sqrt(lax.optimization_barrier(jnp.sum(differences * differences, axis=-2, keepdims=True)) + NORM_EPS)

def outlook_derivative(realization_outlook, truth_field, cell_surface_share):
    realization_list = realization_outlook.shape[0]
    polarity_unit = unit_scaled_lines(realization_outlook - truth_field[None])

    def lone_realization(shard_lines):
        return lax.optimization_barrier(jnp.sum(unit_scaled_lines(shard_lines[None] - realization_outlook), axis=0))
    couple_total = lax.map(lone_realization, realization_outlook)
    weight = LOSS_SCALE * cell_surface_share[None, None, :]
    return weight * (polarity_unit / realization_list - (1.0 - FAIR_EPS) / (realization_list * (realization_list - 1)) * couple_total)

def quantized_entries(numbers):
    return lax.optimization_barrier(numbers.astype(jnp.bfloat16)).astype(jnp.float32)

def tile_grads(queries, grad_rows, log_sums, row_delta, key_tile, value_tile, score_scale):
    scores = jnp.einsum('rhd,khd->hrk', queries, key_tile) * score_scale
    probability = jnp.exp(scores - log_sums[:, :, None])
    dprobs = jnp.einsum('rhd,khd->hrk', grad_rows, value_tile)
    dscores = quantized_entries(probability * (dprobs - row_delta[:, :, None]))
    query_grad = (score_scale * jnp.einsum('hrk,khd->rhd', dscores, key_tile)).astype(jnp.bfloat16)
    key_grad = (score_scale * jnp.einsum('hrk,rhd->khd', dscores, queries)).astype(jnp.bfloat16)
    value_grad = jnp.einsum('hrk,rhd->khd', quantized_entries(probability), grad_rows).astype(jnp.bfloat16)
    return (query_grad, key_grad, value_grad)

def member_grads(arrays, kv_owner, kv_local):
    query, key_rows, value_rows, grad_output, saved_output, row_lse = arrays
    head_count = row_lse.shape[0]
    model_width = query.shape[1]
    head_dim = model_width // head_count
    score_scale = head_dim ** (-0.5)
    split_shape = (SHARDS, NODE_DEV, head_count, head_dim)
    query_blocks = query.astype(jnp.float32).reshape(split_shape)
    grad_blocks = grad_output.astype(jnp.float32).reshape(split_shape)
    saved_blocks = saved_output.astype(jnp.float32).reshape(split_shape)
    row_delta = lax.optimization_barrier(jnp.sum(grad_blocks * saved_blocks, axis=-1)).transpose(0, 2, 1)
    lse_blocks = row_lse.reshape(head_count, SHARDS, NODE_DEV).transpose(1, 0, 2)
    key_blocks = key_rows.astype(jnp.float32).reshape(SHARDS * KBLK_DEV, KB, head_count, head_dim)
    value_blocks = value_rows.astype(jnp.float32).reshape(SHARDS * KBLK_DEV, KB, head_count, head_dim)
    block_ids = (kv_owner * KBLK_DEV + kv_local).astype(jnp.int32)
    zero_grads = jnp.zeros(key_blocks.shape, jnp.float32)

    def per_shard(grads_carry, inputs):
        queries, grad_rows, log_sums, deltas, indices = inputs

        def per_block(running, block_id):
            query_sum, key_grads, value_grads = running
            query_grad, key_grad, value_grad = tile_grads(queries, grad_rows, log_sums, deltas, key_blocks[block_id], value_blocks[block_id], score_scale)
            key_grads = key_grads.at[block_id].add(key_grad.astype(jnp.float32))
            value_grads = value_grads.at[block_id].add(value_grad.astype(jnp.float32))
            return ((query_sum + query_grad.astype(jnp.float32), key_grads, value_grads), None)
        initial = (jnp.zeros(queries.shape, jnp.float32), grads_carry[0], grads_carry[1])
        (query_sum, key_grads, value_grads), unused = lax.scan(per_block, initial, indices)
        return ((key_grads, value_grads), query_sum)
    (key_grads, value_grads), query_sums = lax.scan(per_shard, (zero_grads, zero_grads), (query_blocks, grad_blocks, lse_blocks, row_delta, block_ids))
    return (query_sums.reshape(NODES, model_width), key_grads.reshape(NODES, model_width), value_grads.reshape(NODES, model_width))

def reference(hidden_embedding, decoder_matrix, baseline_field, truth_field, cell_surface_share, node_order, query, key_rows, value_rows, row_lse, kv_owner, kv_local):
    full_coefficient = decoder_matrix.astype(jnp.float32)
    realization_outlook = baseline_field[None] + jnp.einsum('mou,ut->mto', hidden_embedding.astype(jnp.float32), full_coefficient)
    estimate_derivative = quantized_entries(outlook_derivative(realization_outlook, truth_field, cell_surface_share))
    latent_gradient = jnp.einsum('jof,io->jfi', estimate_derivative, full_coefficient).astype(jnp.bfloat16)
    node_index = (node_order + NODE_DEV * jnp.arange(SHARDS, dtype=jnp.int32)[:, None]).reshape(-1).astype(jnp.int32)
    grad_output = jnp.take(latent_gradient, node_index, axis=1)
    saved_output = jnp.take(hidden_embedding, node_index, axis=1)

    def run_member(arrays):
        return member_grads(arrays, kv_owner, kv_local)
    query_grads, key_grads, value_grads = lax.map(run_member, (query, key_rows, value_rows, grad_output, saved_output, row_lse))
    return (query_grads, key_grads, value_grads)
```

```python
import functools

import jax
import jax.numpy as jnp
from jax import lax
from jax.experimental import pallas as pl
from jax.experimental.pallas import tpu as pltpu
from jax.sharding import PartitionSpec as P

KB = 128
LOSS_SCALE = 4096.0
FAIR_EPS = 0.05
NORM_EPS = 1e-06


NN = (((1,), (0,)), ((), ()))
NT = (((1,), (1,)), ((), ()))
TN = (((0,), (0,)), ((), ()))


def dot(a, b, dims):
    return lax.dot_general(a, b, dims, preferred_element_type=jnp.float32)


def unit_scaled_lines(differences):
    return differences * lax.rsqrt(
        jnp.sum(differences * differences, axis=-2, keepdims=True) + NORM_EPS
    )


def listed_block(me_ref, owner_ref, local_ref, half, r, q):
    me = me_ref[0]
    base = (me // half) * half
    s = base + ((me - base) ^ r) + q * half
    s = jnp.where(s >= 2 * half, s - 2 * half, s)
    found = jnp.int32(0)
    for j in range(owner_ref.shape[1]):
        found = jnp.where(owner_ref[s, j] == me, local_ref[s, j], found)
    return found


def pick_kernel(half, me_ref, owner_ref, local_ref, key_ref, value_ref, *out_refs):
    for r in range(half):
        for q in range(2):
            block = listed_block(me_ref, owner_ref, local_ref, half, r, q)
            out_refs[r][q, 0] = key_ref[0, block]
            out_refs[r][q, 1] = value_ref[0, block]


def pick_blocks(half, member, tables, key_blocks, value_blocks):
    _, blocks, rows, width = key_blocks.shape
    tile = jax.ShapeDtypeStruct((2, 2, rows, width), key_blocks.dtype)
    spec = pl.BlockSpec((1, blocks, rows, width), lambda i, *_: (member, 0, 0, 0))
    return pl.pallas_call(
        functools.partial(pick_kernel, half),
        out_shape=[tile] * half,
        grid_spec=pltpu.PrefetchScalarGridSpec(
            num_scalar_prefetch=3,
            grid=(1,),
            in_specs=[spec, spec],
            out_specs=[pl.BlockSpec(tile.shape, lambda i, *_: (0, 0, 0, 0))] * half,
        ),
        compiler_params=pltpu.CompilerParams(vmem_limit_bytes=24 * 2**20),
        cost_estimate=pl.CostEstimate(flops=10**6, bytes_accessed=3 * 2**20, transcendentals=0),
        name=f"pick{member}",
    )(*tables, key_blocks, value_blocks)


def tile_kernel(half, heads, *refs):
    tiles, refs = refs[:half], refs[half:]
    (own_q, far_q, own_gc, far_gc, own_lse, far_lse, own_delta, far_delta, decoder), refs = refs[:9], refs[9:]
    outs, refs = refs[:half], refs[half:]
    own_dq, far_dq, kv, kv_out, queries, grads, lse, delta, total = refs
    step = pl.program_id(0)
    r = lax.rem(step, half)
    far = step < half
    width = queries.shape[1]
    dim = width // heads
    pair = 2 * dim
    scale = dim ** (-0.5)
    rows = kv.shape[1]

    def enter(q_ref, gc_ref, lse_ref, delta_ref):
        queries[...] = q_ref[...]
        grads[...] = dot(decoder[...], gc_ref[...], NN).astype(jnp.bfloat16)
        lse[...] = lse_ref[...]
        delta[...] = delta_ref[...]
        total[...] = jnp.zeros_like(total)

    @pl.when(step == 0)
    def _():
        enter(far_q, far_gc, far_lse, far_delta)

    @pl.when(step == half)
    def _():
        enter(own_q, own_gc, own_lse, own_delta)

    which = jnp.where(far, 1, 0)
    for i in range(half):

        @pl.when(r == i)
        def _():
            kv[...] = tiles[i][which]

    low = lax.broadcasted_iota(jnp.int32, (rows, pair), 1) < dim
    for p in range(heads // 2):
        lanes = pl.ds(p * pair, pair)
        key = kv[0, :, lanes]
        value = kv[1, :, lanes]
        nought = jnp.zeros_like(key)
        keys = jnp.concatenate([jnp.where(low, key, nought), jnp.where(low, nought, key)], axis=0)
        values = jnp.concatenate(
            [jnp.where(low, value, nought), jnp.where(low, nought, value)], axis=0
        )
        q_pair = queries[:, lanes]
        g_pair = grads[lanes, :]
        scores = dot(keys, q_pair, NT)
        dprobs = dot(values, g_pair, NN)
        prob, dscore = [], []
        for k in range(2):
            part = slice(k * rows, (k + 1) * rows)
            h = 2 * p + k
            pr = jnp.exp(scores[part] * scale - lse[pl.ds(h, 1), :])
            prob.append(pr.astype(jnp.bfloat16))
            dscore.append((pr * (dprobs[part] - delta[pl.ds(h, 1), :])).astype(jnp.bfloat16))
        prob = jnp.concatenate(prob, axis=0)
        dscore = jnp.concatenate(dscore, axis=0)
        dv = dot(prob, g_pair, NT)
        dk = dot(dscore, q_pair, NN) * scale
        kv_out[0, :, lanes] = jnp.where(low, dk[:rows], dk[rows:]).astype(jnp.bfloat16)
        kv_out[1, :, lanes] = jnp.where(low, dv[:rows], dv[rows:]).astype(jnp.bfloat16)
        total[lanes, :] += dot(keys, dscore, TN)

    for i in range(half):

        @pl.when(r == i)
        def _():
            outs[i][which] = kv_out[...]

    @pl.when(step == half - 1)
    def _():
        far_dq[...] = (total[...] * scale).T.astype(far_dq.dtype)

    @pl.when(step == 2 * half - 1)
    def _():
        own_dq[...] = (total[...] * scale).T


def tile_grads(half, heads, member, tiles, operands):
    rows, width = operands[0].shape
    kb = tiles[0].shape[2]
    chans = operands[2].shape[0]
    arrays = (*tiles, *operands)
    whole = lambda a: pl.BlockSpec(a.shape, lambda i, nd=len(a.shape): (0,) * nd)
    tile = jax.ShapeDtypeStruct(tiles[0].shape, jnp.bfloat16)
    out_shape = [tile] * half + [
        jax.ShapeDtypeStruct((rows, width), jnp.float32),
        jax.ShapeDtypeStruct((rows, width), jnp.bfloat16),
    ]
    flops = 2 * half * 10 * rows * kb * width
    return pl.pallas_call(
        functools.partial(tile_kernel, half, heads),
        grid=(2 * half,),
        out_shape=out_shape,
        in_specs=[whole(a) for a in arrays],
        out_specs=[whole(a) for a in out_shape],
        scratch_shapes=[
            pltpu.VMEM((2, kb, width), jnp.bfloat16),
            pltpu.VMEM((2, kb, width), jnp.bfloat16),
            pltpu.VMEM((rows, width), jnp.bfloat16),
            pltpu.VMEM((width, rows), jnp.bfloat16),
            pltpu.VMEM((heads, rows), jnp.float32),
            pltpu.VMEM((heads, rows), jnp.float32),
            pltpu.VMEM((width, rows), jnp.float32),
        ],
        compiler_params=pltpu.CompilerParams(
            vmem_limit_bytes=40 * 2**20, dimension_semantics=("arbitrary",)
        ),
        cost_estimate=pl.CostEstimate(
            flops=flops, bytes_accessed=8 * 2**20, transcendentals=2 * half * heads * rows * kb
        ),
        name=f"tiles{member}",
    )(*arrays)


def collect_kernel(half, me_ref, owner_ref, local_ref, *refs):
    parts, refs = refs[:half], refs[half:]
    own_dq, far_dq = refs[:2]
    gq, gk, gv = refs[-3:]
    gq[0] = own_dq[...] + far_dq[...].astype(jnp.float32)
    gk[...] = jnp.zeros_like(gk)
    gv[...] = jnp.zeros_like(gv)
    for r in range(half):
        for q in range(2):
            block = listed_block(me_ref, owner_ref, local_ref, half, r, q)
            gk[0, block] += parts[r][q, 0].astype(jnp.float32)
            gv[0, block] += parts[r][q, 1].astype(jnp.float32)


def collect(half, member, members, blocks, tables, parts, own_dq, far_dq, before):
    rows, width = own_dq.shape
    kb = parts[0].shape[2]
    steps = 4
    part_spec = pl.BlockSpec((2, 2, kb // steps, width), lambda i, *_: (0, 0, i, 0))
    q_spec = pl.BlockSpec((rows // steps, width), lambda i, *_: (i, 0))
    out_shape = [
        jax.ShapeDtypeStruct((members, rows, width), jnp.float32),
        jax.ShapeDtypeStruct((members, blocks, kb, width), jnp.float32),
        jax.ShapeDtypeStruct((members, blocks, kb, width), jnp.float32),
    ]
    kv_spec = pl.BlockSpec((1, blocks, kb // steps, width), lambda i, *_: (member, 0, i, 0))
    extra = () if before is None else tuple(before)
    first = 3 + half + 2
    return pl.pallas_call(
        functools.partial(collect_kernel, half),
        out_shape=out_shape,
        grid_spec=pltpu.PrefetchScalarGridSpec(
            num_scalar_prefetch=3,
            grid=(steps,),
            in_specs=[part_spec] * half
            + [q_spec, q_spec]
            + [pl.BlockSpec(memory_space=pl.ANY)] * len(extra),
            out_specs=[
                pl.BlockSpec((1, rows // steps, width), lambda i, *_: (member, i, 0)),
                kv_spec,
                kv_spec,
            ],
        ),
        input_output_aliases={first + k: k for k in range(len(extra))},
        compiler_params=pltpu.CompilerParams(vmem_limit_bytes=24 * 2**20),
        cost_estimate=pl.CostEstimate(flops=10**6, bytes_accessed=6 * 2**20, transcendentals=0),
        name=f"collect{member}",
    )(*tables, *parts, own_dq, far_dq, *extra)


def shards(
    groups,
    n,
    hidden_embedding,
    decoder_matrix,
    baseline_field,
    truth_field,
    cell_surface_share,
    node_order,
    query,
    key_rows,
    value_rows,
    row_lse,
    kv_owner,
    kv_local,
):
    members, nodes, width = hidden_embedding.shape
    heads = row_lse.shape[1]
    half = n // 2
    blocks = nodes // KB
    me = jnp.full((1,), lax.axis_index("mesh"), jnp.int32)
    tables = (me, kv_owner, kv_local)
    partner = [(s, (s + half) % n) for s in range(n)]
    hop = lambda r: [(s, (s // half) * half + ((s % half) ^ r)) for s in range(n)]

    split = (members, blocks, KB, width)
    key_blocks = key_rows.reshape(split)
    value_blocks = value_rows.reshape(split)
    sent = [pick_blocks(half, m, tables, key_blocks, value_blocks) for m in range(members)]
    far_query = [None] * members
    tiles = [None] * members
    for m in range(members):
        tiles[m] = [sent[m][0]] + [
            lax.ppermute(sent[m][r], "mesh", hop(r)) for r in range(half - 1, 0, -1)
        ][::-1]
        far_query[m] = lax.ppermute(query[m], "mesh", partner)
    far_lse = lax.ppermute(row_lse, "mesh", partner)

    outlook = baseline_field[None] + jnp.einsum(
        "mou,ut->mto", hidden_embedding, decoder_matrix, preferred_element_type=jnp.float32
    )
    others = [outlook] + [
        lax.ppermute(outlook, "member", [(g, (g + k) % groups) for g in range(groups)])
        for k in range(1, groups)
    ]
    total_members = members * groups
    couple = 0.0
    for other in others:
        couple = couple + jnp.sum(
            unit_scaled_lines(outlook[:, None] - other[None]), axis=1
        )
    polarity = unit_scaled_lines(outlook - truth_field[None])
    weight = LOSS_SCALE * cell_surface_share[None, None, :]
    derivative = (
        weight
        * (
            polarity / total_members
            - (1.0 - FAIR_EPS) / (total_members * (total_members - 1)) * couple
        )
    ).astype(jnp.bfloat16)

    permuter = (node_order[0][:, None] == jnp.arange(nodes, dtype=jnp.int32)[None, :]).astype(
        jnp.bfloat16
    )
    columns = jnp.einsum(
        "mcg,tg->mct", derivative, permuter, preferred_element_type=jnp.float32
    ).astype(jnp.bfloat16)
    grad_t = jnp.einsum(
        "wc,mct->mwt", decoder_matrix, columns, preferred_element_type=jnp.float32
    ).astype(jnp.bfloat16)
    saved_t = jnp.einsum(
        "mgw,tg->mwt", hidden_embedding, permuter, preferred_element_type=jnp.float32
    ).astype(jnp.bfloat16)
    by_head = (members, heads, width // heads, nodes)
    delta = jnp.sum(
        grad_t.reshape(by_head).astype(jnp.float32) * saved_t.reshape(by_head).astype(jnp.float32),
        axis=2,
    )
    far_columns = lax.ppermute(columns, "mesh", partner)
    far_delta = lax.ppermute(delta, "mesh", partner)

    result = None
    parts, own, far = [], [], []
    for m in range(members):
        out = tile_grads(
            half,
            heads,
            m,
            tiles[m],
            (
                query[m],
                far_query[m],
                columns[m],
                far_columns[m],
                row_lse[m],
                far_lse[m],
                delta[m],
                far_delta[m],
                decoder_matrix,
            ),
        )
        returned, own_dq, far_dq = out[:half], out[half], out[half + 1]
        parts.append(
            [returned[0]] + [lax.ppermute(returned[r], "mesh", hop(r)) for r in range(1, half)]
        )
        own.append(own_dq)
        far.append(lax.ppermute(far_dq, "mesh", partner))
    for m in range(members):
        result = collect(half, m, members, blocks, tables, parts[m], own[m], far[m], result)
    grad_query, grad_key, grad_value = result
    return (grad_query, grad_key.reshape(key_rows.shape), grad_value.reshape(value_rows.shape))


def solution(mesh):
    rows = P("member", "mesh", None)
    return jax.shard_map(
        functools.partial(shards, mesh.shape["member"], mesh.shape["mesh"]),
        mesh=mesh,
        in_specs=(
            rows,
            P(),
            P(None, "mesh"),
            P(None, "mesh"),
            P("mesh"),
            P("mesh", None),
            rows,
            rows,
            rows,
            P("member", None, "mesh"),
            P(),
            P(),
        ),
        out_specs=(rows, rows, rows),
        check_vma=False,
    )
```

```python
import functools

import jax
import jax.numpy as jnp
from jax import lax
from jax.experimental import pallas as pl
from jax.experimental.pallas import tpu as pltpu
from jax.sharding import PartitionSpec as P

KB = 128
LOSS_SCALE = 4096.0
FAIR_EPS = 0.05
NORM_EPS = 1e-06


NN = (((1,), (0,)), ((), ()))
NT = (((1,), (1,)), ((), ()))
TN = (((0,), (0,)), ((), ()))


def dot(a, b, dims):
    return lax.dot_general(a, b, dims, preferred_element_type=jnp.float32)


def unit_scaled_lines(differences):
    return differences * lax.rsqrt(
        jnp.sum(differences * differences, axis=-2, keepdims=True) + NORM_EPS
    )


def listed_block(me_ref, owner_ref, local_ref, half, r, q):
    me = me_ref[0]
    base = (me // half) * half
    s = base + ((me - base) ^ r) + q * half
    s = jnp.where(s >= 2 * half, s - 2 * half, s)
    found = jnp.int32(0)
    for j in range(owner_ref.shape[1]):
        found = jnp.where(owner_ref[s, j] == me, local_ref[s, j], found)
    return found


def pick_kernel(half, me_ref, owner_ref, local_ref, query_ref, key_ref, value_ref, *refs):
    out_refs = refs[-half - 1 :]
    out_refs[half][...] = query_ref[0]
    for r in range(half):
        for q in range(2):
            block = listed_block(me_ref, owner_ref, local_ref, half, r, q)
            out_refs[r][q, 0] = key_ref[0, block]
            out_refs[r][q, 1] = value_ref[0, block]


def pick_blocks(half, member, tables, query, key_blocks, value_blocks, after):
    _, blocks, rows, width = key_blocks.shape
    nodes = query.shape[1]
    tile = jax.ShapeDtypeStruct((2, 2, rows, width), key_blocks.dtype)
    spec = pl.BlockSpec((1, blocks, rows, width), lambda i, *_: (member, 0, 0, 0))
    return pl.pallas_call(
        functools.partial(pick_kernel, half),
        out_shape=[tile] * half + [jax.ShapeDtypeStruct((nodes, width), query.dtype)],
        grid_spec=pltpu.PrefetchScalarGridSpec(
            num_scalar_prefetch=3,
            grid=(1,),
            in_specs=[pl.BlockSpec((1, nodes, width), lambda i, *_: (member, 0, 0)), spec, spec]
            + [pl.BlockSpec(memory_space=pl.ANY)] * len(after),
            out_specs=[pl.BlockSpec(tile.shape, lambda i, *_: (0, 0, 0, 0))] * half
            + [pl.BlockSpec((nodes, width), lambda i, *_: (0, 0))],
        ),
        compiler_params=pltpu.CompilerParams(vmem_limit_bytes=24 * 2**20),
        cost_estimate=pl.CostEstimate(flops=10**6, bytes_accessed=3 * 2**20, transcendentals=0),
        name=f"pick{member}",
    )(*tables, query, key_blocks, value_blocks, *after)


def tile_kernel(half, heads, *refs):
    tiles, refs = refs[:half], refs[half:]
    (own_q, far_q, own_gc, far_gc, own_terms, far_terms, decoder), refs = refs[:7], refs[7:]
    outs, refs = refs[:half], refs[half:]
    own_dq, far_dq, kv, kv_out, queries, grads, terms, total = refs
    step = pl.program_id(0)
    r = lax.rem(step, half)
    far = step < half
    width = queries.shape[1]
    dim = width // heads
    pair = 2 * dim
    scale = dim ** (-0.5)
    rows = kv.shape[1]

    def enter(q_ref, gc_ref, terms_ref):
        queries[...] = q_ref[...]
        grads[...] = dot(decoder[...], gc_ref[...], NN).astype(jnp.bfloat16)
        terms[...] = terms_ref[...]
        total[...] = jnp.zeros_like(total)

    @pl.when(step == 0)
    def _():
        enter(far_q, far_gc, far_terms)

    @pl.when(step == half)
    def _():
        enter(own_q, own_gc, own_terms)

    which = jnp.where(far, 1, 0)
    for i in range(half):

        @pl.when(r == i)
        def _():
            kv[...] = tiles[i][which]

    low = lax.broadcasted_iota(jnp.int32, (rows, pair), 1) < dim
    for p in range(heads // 2):
        lanes = pl.ds(p * pair, pair)
        key = kv[0, :, lanes]
        value = kv[1, :, lanes]
        nought = jnp.zeros_like(key)
        keys = jnp.concatenate([jnp.where(low, key, nought), jnp.where(low, nought, key)], axis=0)
        values = jnp.concatenate(
            [jnp.where(low, value, nought), jnp.where(low, nought, value)], axis=0
        )
        q_pair = queries[:, lanes]
        g_pair = grads[lanes, :]
        scores = dot(keys, q_pair, NT)
        dprobs = dot(values, g_pair, NN)
        prob, dscore = [], []
        for k in range(2):
            part = slice(k * rows, (k + 1) * rows)
            h = 2 * p + k
            pr = jnp.exp(scores[part] * scale - terms[pl.ds(h, 1), :])
            prob.append(pr.astype(jnp.bfloat16))
            dscore.append((pr * (dprobs[part] - terms[pl.ds(heads + h, 1), :])).astype(jnp.bfloat16))
        prob = jnp.concatenate(prob, axis=0)
        dscore = jnp.concatenate(dscore, axis=0)
        dv = dot(prob, g_pair, NT)
        dk = dot(dscore, q_pair, NN) * scale
        kv_out[0, :, lanes] = jnp.where(low, dk[:rows], dk[rows:]).astype(jnp.bfloat16)
        kv_out[1, :, lanes] = jnp.where(low, dv[:rows], dv[rows:]).astype(jnp.bfloat16)
        total[lanes, :] += dot(keys, dscore, TN)

    for i in range(half):

        @pl.when(r == i)
        def _():
            outs[i][which] = kv_out[...]

    @pl.when(step == half - 1)
    def _():
        far_dq[...] = (total[...] * scale).T.astype(far_dq.dtype)

    @pl.when(step == 2 * half - 1)
    def _():
        own_dq[...] = (total[...] * scale).T


def tile_grads(half, heads, member, tiles, operands):
    rows, width = operands[0].shape
    kb = tiles[0].shape[2]
    chans = operands[2].shape[0]
    arrays = (*tiles, *operands)
    whole = lambda a: pl.BlockSpec(a.shape, lambda i, nd=len(a.shape): (0,) * nd)
    tile = jax.ShapeDtypeStruct(tiles[0].shape, jnp.bfloat16)
    out_shape = [tile] * half + [
        jax.ShapeDtypeStruct((rows, width), jnp.float32),
        jax.ShapeDtypeStruct((rows, width), jnp.bfloat16),
    ]
    flops = 2 * half * 10 * rows * kb * width
    return pl.pallas_call(
        functools.partial(tile_kernel, half, heads),
        grid=(2 * half,),
        out_shape=out_shape,
        in_specs=[whole(a) for a in arrays],
        out_specs=[whole(a) for a in out_shape],
        scratch_shapes=[
            pltpu.VMEM((2, kb, width), jnp.bfloat16),
            pltpu.VMEM((2, kb, width), jnp.bfloat16),
            pltpu.VMEM((rows, width), jnp.bfloat16),
            pltpu.VMEM((width, rows), jnp.bfloat16),
            pltpu.VMEM((2 * heads, rows), jnp.float32),
            pltpu.VMEM((width, rows), jnp.float32),
        ],
        compiler_params=pltpu.CompilerParams(
            vmem_limit_bytes=40 * 2**20, dimension_semantics=("arbitrary",)
        ),
        cost_estimate=pl.CostEstimate(
            flops=flops, bytes_accessed=8 * 2**20, transcendentals=2 * half * heads * rows * kb
        ),
        name=f"tiles{member}",
    )(*arrays)


def collect_kernel(half, me_ref, owner_ref, local_ref, *refs):
    parts, refs = refs[:half], refs[half:]
    own_dq, far_dq = refs[:2]
    gq, gk, gv = refs[-3:]
    gq[0] = own_dq[...] + far_dq[...].astype(jnp.float32)
    gk[...] = jnp.zeros_like(gk)
    gv[...] = jnp.zeros_like(gv)
    for r in range(half):
        for q in range(2):
            block = listed_block(me_ref, owner_ref, local_ref, half, r, q)
            gk[0, block] += parts[r][q, 0].astype(jnp.float32)
            gv[0, block] += parts[r][q, 1].astype(jnp.float32)


def collect(half, member, members, blocks, tables, parts, own_dq, far_dq, before):
    rows, width = own_dq.shape
    kb = parts[0].shape[2]
    steps = 4
    part_spec = pl.BlockSpec((2, 2, kb // steps, width), lambda i, *_: (0, 0, i, 0))
    q_spec = pl.BlockSpec((rows // steps, width), lambda i, *_: (i, 0))
    out_shape = [
        jax.ShapeDtypeStruct((members, rows, width), jnp.float32),
        jax.ShapeDtypeStruct((members, blocks, kb, width), jnp.float32),
        jax.ShapeDtypeStruct((members, blocks, kb, width), jnp.float32),
    ]
    kv_spec = pl.BlockSpec((1, blocks, kb // steps, width), lambda i, *_: (member, 0, i, 0))
    extra = () if before is None else tuple(before)
    first = 3 + half + 2
    return pl.pallas_call(
        functools.partial(collect_kernel, half),
        out_shape=out_shape,
        grid_spec=pltpu.PrefetchScalarGridSpec(
            num_scalar_prefetch=3,
            grid=(steps,),
            in_specs=[part_spec] * half
            + [q_spec, q_spec]
            + [pl.BlockSpec(memory_space=pl.ANY)] * len(extra),
            out_specs=[
                pl.BlockSpec((1, rows // steps, width), lambda i, *_: (member, i, 0)),
                kv_spec,
                kv_spec,
            ],
        ),
        input_output_aliases={first + k: k for k in range(len(extra))},
        compiler_params=pltpu.CompilerParams(vmem_limit_bytes=24 * 2**20),
        cost_estimate=pl.CostEstimate(flops=10**6, bytes_accessed=6 * 2**20, transcendentals=0),
        name=f"collect{member}",
    )(*tables, *parts, own_dq, far_dq, *extra)


def shards(
    groups,
    n,
    hidden_embedding,
    decoder_matrix,
    baseline_field,
    truth_field,
    cell_surface_share,
    node_order,
    query,
    key_rows,
    value_rows,
    row_lse,
    kv_owner,
    kv_local,
):
    members, nodes, width = hidden_embedding.shape
    heads = row_lse.shape[1]
    half = n // 2
    blocks = nodes // KB
    me = jnp.full((1,), lax.axis_index("mesh"), jnp.int32)
    tables = (me, kv_owner, kv_local)
    partner = [(s, (s + half) % n) for s in range(n)]
    hop = lambda r: [(s, (s // half) * half + ((s % half) ^ r)) for s in range(n)]

    split = (members, blocks, KB, width)
    key_blocks = key_rows.reshape(split)
    value_blocks = value_rows.reshape(split)
    near_query = [None] * members
    far_query = [None] * members
    tiles = [None] * members

    def forward(m, after):
        *sent, near_query[m] = pick_blocks(
            half, m, tables, query, key_blocks, value_blocks, after
        )
        far_query[m] = lax.ppermute(near_query[m], "mesh", partner)
        tiles[m] = [sent[0]] + [
            lax.ppermute(sent[r], "mesh", hop(r)) for r in range(half - 1, 0, -1)
        ][::-1]

    forward(0, ())
    baseline_field, near_query[0] = lax.optimization_barrier((baseline_field, near_query[0]))

    outlook = baseline_field[None] + jnp.einsum(
        "mou,ut->mto", hidden_embedding, decoder_matrix, preferred_element_type=jnp.float32
    )
    others = [outlook] + [
        lax.ppermute(outlook, "member", [(g, (g + k) % groups) for g in range(groups)])
        for k in range(1, groups)
    ]
    total_members = members * groups
    couple = 0.0
    for other in others:
        couple = couple + jnp.sum(
            unit_scaled_lines(outlook[:, None] - other[None]), axis=1
        )
    polarity = unit_scaled_lines(outlook - truth_field[None])
    weight = LOSS_SCALE * cell_surface_share[None, None, :]
    derivative = (
        weight
        * (
            polarity / total_members
            - (1.0 - FAIR_EPS) / (total_members * (total_members - 1)) * couple
        )
    ).astype(jnp.bfloat16)

    permuter = (node_order[0][:, None] == jnp.arange(nodes, dtype=jnp.int32)[None, :]).astype(
        jnp.bfloat16
    )
    columns = jnp.einsum(
        "mcg,tg->mct", derivative, permuter, preferred_element_type=jnp.float32
    ).astype(jnp.bfloat16)
    grad_t = jnp.einsum(
        "wc,mct->mwt", decoder_matrix, columns, preferred_element_type=jnp.float32
    ).astype(jnp.bfloat16)
    saved_t = jnp.einsum(
        "mgw,tg->mwt", hidden_embedding, permuter, preferred_element_type=jnp.float32
    ).astype(jnp.bfloat16)
    by_head = (members, heads, width // heads, nodes)
    delta = jnp.sum(
        grad_t.reshape(by_head).astype(jnp.float32) * saved_t.reshape(by_head).astype(jnp.float32),
        axis=2,
    )
    far_columns = lax.ppermute(columns, "mesh", partner)
    row_terms = jnp.concatenate([row_lse, delta], axis=1)
    far_terms = lax.ppermute(row_terms, "mesh", partner)
    for m in range(1, members):
        forward(m, (row_terms,))

    result = None
    parts, own, far = [], [], []
    for m in range(members):
        out = tile_grads(
            half,
            heads,
            m,
            tiles[m],
            (
                near_query[m],
                far_query[m],
                columns[m],
                far_columns[m],
                row_terms[m],
                far_terms[m],
                decoder_matrix,
            ),
        )
        returned, own_dq, far_dq = out[:half], out[half], out[half + 1]
        parts.append(
            [returned[0]] + [lax.ppermute(returned[r], "mesh", hop(r)) for r in range(1, half)]
        )
        own.append(own_dq)
        far.append(lax.ppermute(far_dq, "mesh", partner))
    for m in range(members):
        result = collect(half, m, members, blocks, tables, parts[m], own[m], far[m], result)
    grad_query, grad_key, grad_value = result
    return (grad_query, grad_key.reshape(key_rows.shape), grad_value.reshape(value_rows.shape))


def solution(mesh):
    rows = P("member", "mesh", None)
    return jax.shard_map(
        functools.partial(shards, mesh.shape["member"], mesh.shape["mesh"]),
        mesh=mesh,
        in_specs=(
            rows,
            P(),
            P(None, "mesh"),
            P(None, "mesh"),
            P("mesh"),
            P("mesh", None),
            rows,
            rows,
            rows,
            P("member", None, "mesh"),
            P(),
            P(),
        ),
        out_specs=(rows, rows, rows),
        check_vma=False,
    )
```
